256 devices in a mesh: row: 8 (over y_lo, x), col: 32 (over z, y_hi, core).
Axes of the slice: x: 4, y: 4 (y_hi: 2, y_lo: 2; y = y_hi * 2 + y_lo), z: 8, core: 2. Of those that a mesh axis runs over, the one named last changes fastest.
Arguments:
- charge: float32 [256, 256, 256], P('col', 'row'), may hold values from -6 to 6
- green_spectrum: float32 [512, 512, 512], P('row', 'col'), may hold values from 0.2 to 2
Outputs:
- potential: float32 [256, 256, 256], P('col', 'row')
The draws below stay inside these ranges and needn't reach their ends.
All inputs are finite; a program needn't handle non-finite values.
Results may differ from the reference program's by a relative error of at most 0.00007.
Values sent between devices are 32-bit elements; how exact they have to be, the bound alone decides.
A program may use at most 128 MiB of HBM per device.

```python
import math
import jax
import jax.numpy as jnp

M = 512
N = 256


def block_levels(key, shape, shards, low, largest):
    gain, own = 1.0, jax.random.fold_in(key, 6)
    for axis_at, blocks in shards:
        heights = jnp.exp(jax.random.uniform(jax.random.fold_in(own, axis_at), (blocks,), jnp.float32, low / len(shards), largest / len(shards)))
        gain = gain * jnp.repeat(heights, shape[axis_at] // blocks).reshape([-1 if axis == axis_at else 1 for axis in range(len(shape))])
    return gain


def noise(rng, dims, spread, bound, shards=(), held_as=jnp.bfloat16):
    array = jax.random.normal(rng, dims, jnp.float32) * spread
    if len(shards) > 0:
        array = block_levels(rng, dims, shards, -0.22, 0.18) * array
    return jnp.clip(array, min=-bound, max=bound).astype(held_as)


def setup_inputs(seed: int = 0) -> dict:
    seeds = jax.random.split(jax.random.key(seed), 3)
    charge = noise(seeds[0], (N, N, N), 1.0, 6.0, ((0, 32), (1, 8)), jnp.float32)
    green_spectrum = jnp.clip(jnp.exp(math.log(2.0) - 2.3025851 * jax.random.uniform(seeds[1], (M, M, M), jnp.float32) ** block_levels(seeds[1], (M, M, M), ((0, 8), (1, 32)), -0.2, 0.2)), 0.2, 2.0)
    return {"charge": charge, "green_spectrum": green_spectrum}


def reference(charge, green_spectrum):
    spectrum = jnp.fft.fft(charge, n=M, axis=2)
    spectrum = jnp.fft.fft(spectrum, n=M, axis=1)
    spectrum = jnp.fft.fft(spectrum, n=M, axis=0)
    product = spectrum * jnp.transpose(green_spectrum, (2, 1, 0))
    field = jnp.fft.ifft(product, axis=0)[:N]
    field = jnp.fft.ifft(field, axis=1)[:, :N]
    field = jnp.fft.ifft(field, axis=2)[:, :, :N]
    return jnp.real(field).astype(jnp.float32)
```

```python
import functools
import math

import jax
import jax.numpy as jnp
import numpy as np
from jax import lax
from jax.experimental import pallas as pl
from jax.experimental.pallas import tpu as pltpu
from jax.sharding import PartitionSpec as P

M = 512
N = 256
ROWS = 8
COLS = 32
CHUNKS = 4
CW = M // ROWS // CHUNKS
MESH = pl.DeviceIdType.MESH


def halves(table):
    high = table.astype(jnp.bfloat16)
    low = (table - high.astype(np.float32)).astype(jnp.bfloat16)
    return np.stack([high, low])


def tables():
    turns = np.arange(N)[:, None] * np.arange(M)[None, :] % M
    angles = turns * (2.0 * np.pi / M)
    cosine, sine = np.cos(angles), np.sin(angles)
    parts = np.stack([cosine, -sine], 1).reshape(N, 2, ROWS, CHUNKS, CW)
    z_table = parts.transpose(3, 0, 1, 4, 2).reshape(CHUNKS, N, 2 * CW * ROWS)
    full = np.concatenate(
        [np.concatenate([cosine, -sine], 1), np.concatenate([sine, cosine], 1)], 0
    )
    return halves(z_table.astype(np.float32)), halves(full.astype(np.float32))


def split(value):
    high = value.astype(jnp.bfloat16)
    low = (value - high.astype(jnp.float32)).astype(jnp.bfloat16)
    return high, low


def product(left, right, dims):
    def one(a, b):
        return lax.dot_general(a, b, (dims, ((), ())), preferred_element_type=jnp.float32)

    return one(left[0], right[0]) + (one(left[0], right[1]) + one(left[1], right[0]))


def swap_groups(parts, width):
    parts = list(parts)
    count = len(parts)
    lanes = parts[0].shape[-1]
    step = 1
    while step < count:
        shift = step * width
        lane = lax.broadcasted_iota(jnp.int32, parts[0].shape, len(parts[0].shape) - 1)
        upper = (lane // shift) % 2 == 1
        axis = len(parts[0].shape) - 1
        for i in range(count):
            if i & step:
                continue
            one, two = parts[i], parts[i | step]
            parts[i] = jnp.where(upper, pltpu.roll(two, shift, axis), one)
            parts[i | step] = jnp.where(upper, two, pltpu.roll(one, lanes - shift, axis))
        step *= 2
    return parts


def body(
    charge, green, ztab_h, full_h, out, cells, gvm, ztab, full, row_out, row_in, col_out, col_in,
    back_out, back_in, last_out, last_in, load, s_row, r_row, s_col, r_col, s_back, r_back,
    s_last, r_last,
):
    row, col = lax.axis_index("row"), lax.axis_index("col")
    barrier = pltpu.get_barrier_semaphore()
    loads = [
        pltpu.make_async_copy(src, dst, load.at[k])
        for k, (src, dst) in enumerate(
            [(charge, cells), (ztab_h, ztab), (full_h, full), (green, gvm)]
        )
    ]
    for one in loads:
        one.start()

    def row_peer(k):
        return (row + k) % ROWS

    def col_peer(k):
        return (col + k) % COLS

    @pl.loop(1, ROWS)
    def _(k):
        pl.semaphore_signal(barrier, inc=1, device_id={"row": row_peer(k)}, device_id_type=MESH)

    @pl.loop(1, COLS)
    def _(k):
        pl.semaphore_signal(barrier, inc=1, device_id={"col": col_peer(k)}, device_id_type=MESH)

    def send(source, target, s_sem, r_sem, axis, j):
        count, me, peer = (ROWS, row, row_peer) if axis == "row" else (COLS, col, col_peer)

        @pl.loop(1, count)
        def _(k):
            to = peer(k)
            pltpu.make_async_remote_copy(
                src_ref=source.at[j, to],
                dst_ref=target.at[j, me],
                send_sem=s_sem.at[j],
                recv_sem=r_sem.at[j],
                device_id={axis: to},
                device_id_type=MESH,
            ).start()

    def await_all(ref, sem, j):
        view = ref.at[j, pl.ds(0, ref.shape[1] - 1)]
        pltpu.make_async_copy(view, view, sem.at[j]).wait()

    loads[0].wait()
    loads[1].wait()
    cells_h, cells_l = split(cells[...].reshape(8 * 32, N))
    pl.semaphore_wait(barrier, ROWS - 1 + COLS - 1)

    @pl.loop(0, CHUNKS)
    def _(j):
        along_z = product((cells_h, cells_l), (ztab[0, j], ztab[1, j]), ((1,), (0,)))
        for q in range(2):
            block = along_z[:, q * 128 : q * 128 + 128]
            pieces = swap_groups([block[x * 32 : x * 32 + 32] for x in range(8)], 1)
            for r in range(ROWS):
                row_out[j, r, q] = pieces[r]
        row_in[j, row] = row_out[j, row]
        send(row_out, row_in, s_row, r_row, "row", j)

    loads[2].wait()

    @pl.loop(0, CHUNKS)
    def _(j):
        await_all(row_in, r_row, j)
        data = jnp.concatenate([row_in[j, :, q].reshape(N, 128) for q in range(2)], 0)
        along_y = product(split(data.T), (full[0], full[1]), ((1,), (0,)))
        along_y = along_y.reshape(2, 8, 8, 2 * M)
        for v in range(8):
            q, high = v // 4, v % 4
            block = along_y[..., v * 128 : v * 128 + 128]
            pieces = swap_groups([block[:, i].reshape(16, 128) for i in range(8)], 16)
            for low in range(8):
                col_out[j, high * 8 + low, q] = pieces[low].reshape(2, 8, 128)
        col_in[j, col] = col_out[j, col]
        send(col_out, col_in, s_col, r_col, "col", j)

    loads[3].wait()

    @pl.loop(0, CHUNKS)
    def _(j):
        await_all(col_in, r_col, j)
        halves_x = []
        for h in range(2):
            data = jnp.concatenate([col_in[j, :, q, h].reshape(N, 128) for q in range(2)], 0)
            spectrum = product(split(data.T), (full[0], full[1]), ((1,), (0,)))
            weight = gvm[pl.ds(j * CW + h * 8, 8)].reshape(128, M)
            scaled = spectrum * jnp.concatenate([weight, weight], 1)
            halves_x.append(product(split(scaled), (full[0], full[1]), ((1,), (1,))))
        for v in range(4):
            q, high = v // 2, v % 2
            pieces = swap_groups(
                [
                    halves_x[i // 8][(i % 8) * 16 : (i % 8) * 16 + 16, v * 128 : v * 128 + 128]
                    for i in range(16)
                ],
                8,
            )
            for low in range(16):
                back_out[j, high * 16 + low, q] = pieces[low]
        back_in[j, col] = back_out[j, col]
        send(back_out, back_in, s_back, r_back, "col", j)

    @pl.loop(0, CHUNKS)
    def _(j):
        await_all(back_in, r_back, j)
        data = jnp.concatenate([back_in[j, :, q].reshape(M, 128) for q in range(2)], 0)
        back_y = product((full[0], full[1]), split(data), ((1,), (0,)))
        for q in range(2):
            for r in range(ROWS):
                last_out[j, r, q] = back_y[q * N + r * 32 : q * N + r * 32 + 32]
        last_in[j, row] = last_out[j, row]
        send(last_out, last_in, s_last, r_last, "row", j)

    out[...] = jnp.zeros_like(out)

    @pl.loop(0, CHUNKS)
    def _(j):
        await_all(last_in, r_last, j)
        parts = []
        for q in range(2):
            pieces = swap_groups([last_in[j, r, q] for r in range(ROWS)], 1)
            parts.append(jnp.concatenate(pieces, 0))
        data = jnp.concatenate(parts, 1)
        out[...] += product(split(data), (ztab[0, j], ztab[1, j]), ((1,), (1,)))

    @pl.loop(0, CHUNKS)
    def _(j):
        await_all(row_out, s_row, j)
        await_all(col_out, s_col, j)
        await_all(back_out, s_back, j)
        await_all(last_out, s_last, j)


def on_device(charge, green_spectrum):
    z_table, full_table = tables()
    any_space = pl.BlockSpec(memory_space=pl.ANY)
    field = pl.pallas_call(
        body,
        out_shape=jax.ShapeDtypeStruct((8 * 32, N), jnp.float32),
        in_specs=[any_space] * 4,
        out_specs=pl.BlockSpec(memory_space=pltpu.VMEM),
        scratch_shapes=[
            pltpu.VMEM((8, 32, N), jnp.float32),
            pltpu.VMEM((64, 16, M), jnp.float32),
            pltpu.VMEM(z_table.shape, jnp.bfloat16),
            pltpu.VMEM(full_table.shape, jnp.bfloat16),
            pltpu.VMEM((CHUNKS, ROWS, 2, 32, 128), jnp.float32),
            pltpu.VMEM((CHUNKS, ROWS, 2, 32, 128), jnp.float32),
            pltpu.VMEM((CHUNKS, COLS, 2, 2, 8, 128), jnp.float32),
            pltpu.VMEM((CHUNKS, COLS, 2, 2, 8, 128), jnp.float32),
            pltpu.VMEM((CHUNKS, COLS, 2, 16, 128), jnp.float32),
            pltpu.VMEM((CHUNKS, COLS, 2, 16, 128), jnp.float32),
            pltpu.VMEM((CHUNKS, ROWS, 2, 32, 128), jnp.float32),
            pltpu.VMEM((CHUNKS, ROWS, 2, 32, 128), jnp.float32),
            pltpu.SemaphoreType.DMA((4,)),
        ]
        + [pltpu.SemaphoreType.DMA((CHUNKS,))] * 8,
        compiler_params=pltpu.CompilerParams(
            collective_id=0, has_side_effects=True, vmem_limit_bytes=56 * 2**20
        ),
        name="poisson",
    )(charge, green_spectrum, z_table, full_table)
    return (field * (1.0 / M**3)).reshape(8, 32, N)


def solution(mesh):
    in_specs = (P("col", "row", None), P("row", "col", None))
    out_specs = P("col", "row", None)
    return jax.shard_map(
        on_device, mesh=mesh, in_specs=in_specs, out_specs=out_specs, check_vma=False
    )
```

```python
import functools
import math

import jax
import jax.numpy as jnp
import numpy as np
from jax import lax
from jax.experimental import pallas as pl
from jax.experimental.pallas import tpu as pltpu
from jax.sharding import PartitionSpec as P

M = 512
N = 256
ROWS = 8
COLS = 32
CHUNKS = 4
CW = M // ROWS // CHUNKS
MESH = pl.DeviceIdType.MESH


def halves(table):
    high = table.astype(jnp.bfloat16)
    low = (table - high.astype(np.float32)).astype(jnp.bfloat16)
    return np.stack([high, low])


def tables():
    turns = np.arange(N)[:, None] * np.arange(M)[None, :] % M
    angles = turns * (2.0 * np.pi / M)
    cosine, sine = np.cos(angles), np.sin(angles)
    parts = np.stack([cosine, -sine], 1).reshape(N, 2, ROWS, 2, CW, 2)
    z_table = parts.transpose(5, 3, 0, 1, 4, 2).reshape(CHUNKS, N, 2 * CW * ROWS)
    order = np.arange(N).reshape(ROWS, 2, CW).transpose(1, 2, 0).reshape(N)
    gap = 2 * (order[None, :] - order[:, None]) + 1
    bridge = 2.0 / N / (1.0 - np.exp(-2j * np.pi * gap / M))
    return (
        halves(z_table.astype(np.float32)),
        halves(np.stack([cosine, sine]).astype(np.float32)),
        halves(np.stack([bridge.real, bridge.imag]).astype(np.float32)),
    )


def split(value):
    high = value.astype(jnp.bfloat16)
    low = (value - high.astype(jnp.float32)).astype(jnp.bfloat16)
    return high, low


def product(left, right, dims):
    def one(a, b):
        return lax.dot_general(a, b, (dims, ((), ())), preferred_element_type=jnp.float32)

    return one(left[0], right[0]) + (one(left[0], right[1]) + one(left[1], right[0]))


def swap_groups(parts, width):
    parts = list(parts)
    count = len(parts)
    lanes = parts[0].shape[-1]
    step = 1
    while step < count:
        shift = step * width
        lane = lax.broadcasted_iota(jnp.int32, parts[0].shape, len(parts[0].shape) - 1)
        upper = (lane // shift) % 2 == 1
        axis = len(parts[0].shape) - 1
        for i in range(count):
            if i & step:
                continue
            one, two = parts[i], parts[i | step]
            parts[i] = jnp.where(upper, pltpu.roll(two, shift, axis), one)
            parts[i | step] = jnp.where(upper, two, pltpu.roll(one, lanes - shift, axis))
        step *= 2
    return parts


def body(
    charge, green, ztab_h, wave_h, bridge_h, out, cells, gvm, ztab, full, bridge,
    row_out, row_in, col_out, col_in, back_out, back_in, last_out, last_in,
    even_in, odd_out, odd_in, even_out, fold_in, load,
    s_row, r_row, s_col, r_col, s_back, r_back, s_last, r_last,
    s_even, r_even, s_odd, r_odd, s_fold, r_fold, s_ret, r_ret,
):
    row, col = lax.axis_index("row"), lax.axis_index("col")
    barrier = pltpu.get_barrier_semaphore()
    low, high = pl.ds(0, N), pl.ds(N, N)
    left, right = pl.ds(0, M), pl.ds(M, M)
    pairs = [
        (charge, cells),
        (ztab_h, ztab),
        (wave_h.at[:, 0], full.at[:, low, left]),
        (wave_h.at[:, 0], full.at[:, high, right]),
        (wave_h.at[:, 1], full.at[:, high, left]),
        (bridge_h.at[:, 0], bridge.at[:, low, low]),
        (bridge_h.at[:, 0], bridge.at[:, high, high]),
        (bridge_h.at[:, 1], bridge.at[:, low, high]),
        (green, gvm),
    ]
    loads = [
        pltpu.make_async_copy(src, dst, load.at[k]) for k, (src, dst) in enumerate(pairs)
    ]

    def row_peer(k):
        return (row + k) % ROWS

    def col_peer(k):
        return (col + k) % COLS

    @pl.loop(1, COLS)
    def _(k):
        pl.semaphore_signal(barrier, inc=1, device_id={"col": col_peer(k)}, device_id_type=MESH)

    @pl.loop(1, ROWS)
    def _(k):
        pl.semaphore_signal(barrier, inc=1, device_id={"row": row_peer(k)}, device_id_type=MESH)

    for one in loads:
        one.start()

    def send_row(source, target, s_sem, r_sem):
        @pl.loop(1, ROWS)
        def _(k):
            to = row_peer(k)
            pltpu.make_async_remote_copy(
                src_ref=source(to),
                dst_ref=target,
                send_sem=s_sem,
                recv_sem=r_sem,
                device_id={"row": to},
                device_id_type=MESH,
            ).start()

    def send_col(source, target, s_sem, r_sem, j, half):
        target[j, half, col] = source[j, half, col]

        @pl.loop(1, COLS)
        def _(k):
            to = col_peer(k)
            pltpu.make_async_remote_copy(
                src_ref=source.at[j, half, to],
                dst_ref=target.at[j, half, col],
                send_sem=s_sem.at[2 * j + half],
                recv_sem=r_sem.at[2 * j + half],
                device_id={"col": to},
                device_id_type=MESH,
            ).start()

    def await_bytes(view, sem):
        pltpu.make_async_copy(view, view, sem).wait()

    def await_row(ref, sem, j):
        await_bytes(ref.at[j, pl.ds(0, ROWS - 1)], sem.at[j])

    def await_col(ref, sem, j, half):
        await_bytes(ref.at[j, half, pl.ds(0, COLS - 1)], sem.at[2 * j + half])

    loads[0].wait()
    loads[1].wait()
    cells_h, cells_l = split(cells[...].reshape(8 * 32, N))

    @pl.loop(0, CHUNKS)
    def _(j):
        along_z = product((cells_h, cells_l), (ztab[0, j], ztab[1, j]), ((1,), (0,)))
        for q in range(2):
            block = along_z[:, q * 128 : q * 128 + 128]
            pieces = swap_groups([block[x * 32 : x * 32 + 32] for x in range(8)], 1)
            for r in range(ROWS):
                row_out[j, r, q] = pieces[r]

    pl.semaphore_wait(barrier, ROWS - 1 + COLS - 1)

    @pl.loop(0, CHUNKS)
    def _(j):
        send_row(lambda to: row_out.at[j, to], row_in.at[j, row], s_row.at[j], r_row.at[j])
        row_in[j, row] = row_out[j, row]

    for one in loads[2:8]:
        one.wait()
    full[:, 0:N, M:] = -full[:, N:, 0:M]
    bridge[:, N:, 0:N] = -bridge[:, 0:N, N:]

    @pl.loop(0, CHUNKS)
    def _(j):
        await_row(row_in, r_row, j)
        data = jnp.concatenate([row_in[j, :, q].reshape(N, 128) for q in range(2)], 0)
        along_y = product(split(data.T), (full[0], full[1]), ((1,), (0,)))
        for v in range(8):
            q, top = v // 4, v % 4
            pieces = swap_groups(
                [along_y[i * 8 : i * 8 + 8, v * 128 : v * 128 + 128] for i in range(16)], 8
            )
            for g in range(16):
                col_out[j, g % 2, top * 8 + g // 2, q] = pieces[g]

        @pl.when(j < 2)
        def _():
            send_col(col_out, col_in, s_col, r_col, j, 0)

        @pl.when(j == 1)
        def _():
            send_col(col_out, col_in, s_col, r_col, 0, 1)

        @pl.when(j >= 1)
        def _():
            send_col(col_out, col_in, s_col, r_col, j, 1)

    loads[8].wait()
    for e in range(2):
        back_in[2 + e, 0] = jnp.zeros_like(back_in[2 + e, 0])

    def four(index):
        return pl.ds(index * 4, 4)

    def across(source, target, dims):
        parts = []
        for q in range(2):
            for e in range(2):
                pieces = [source[e, r, :, q].reshape(32, 128) for r in range(ROWS)]
                parts.append(jnp.concatenate(swap_groups(pieces, 1), 0))
        data = jnp.concatenate(parts, 1)
        moved = product(split(data), (bridge[0], bridge[1]), dims)
        for v in range(4):
            q, e = v // 2, v % 2
            block = moved[:, v * 128 : v * 128 + 128]
            pieces = swap_groups([block[k * 32 : k * 32 + 32] for k in range(8)], 1)
            for r in range(ROWS):
                target[e, r, :, q] = pieces[r].reshape(4, 8, 128)

    @pl.loop(0, 2 * CHUNKS)
    def _(s):
        j = s // 4 * 2 + s % 2
        half = s % 4 // 2
        e = s % 2

        @pl.when(s == 3)
        def _():
            for k in range(2):
                await_row(even_in, r_even, k)
            across(even_in, odd_out, ((1,), (0,)))
            for k in range(2):
                send_row(
                    lambda to: odd_out.at[k, to],
                    col_in.at[2 + k, 0, four(row)],
                    s_odd.at[k],
                    r_odd.at[k],
                )
                col_in[2 + k, 0, four(row)] = odd_out[k, row]

        @pl.when((j < 2) | (half == 1))
        def _():
            await_col(col_in, r_col, j, half)

        @pl.when((j >= 2) & (half == 0))
        def _():
            await_row(odd_in, r_odd, e)

        @pl.when(s < 2)
        def _():
            send_row(
                lambda to: col_in.at[e, 0, four(to)],
                even_in.at[e, row],
                s_even.at[e],
                r_even.at[e],
            )
            even_in[e, row] = col_in[e, 0, four(row)]

        data = jnp.concatenate([col_in[j, half, :, q].reshape(N, 128) for q in range(2)], 0)
        spectrum = product(split(data.T), (full[0], full[1]), ((1,), (0,)))
        weight = gvm[pl.ds(e * CW, CW), j // 2, half].reshape(128, M)
        scaled = spectrum * jnp.concatenate([weight, weight], 1)
        along_x = product(split(scaled), (full[0], full[1]), ((1,), (1,)))
        for v in range(4):
            q, top = v // 2, v % 2
            pieces = swap_groups(
                [along_x[i * 8 : i * 8 + 8, v * 128 : v * 128 + 128] for i in range(16)], 8
            )
            for g in range(16):
                back_out[j, half, top * 16 + g, q] = pieces[g]

        @pl.when(half == 1)
        def _():
            send_col(back_out, back_in, s_back, r_back, j, half)

        @pl.when((j >= 2) & (half == 0))
        def _():
            send_row(
                lambda to: back_out.at[j, 0, four(to)],
                odd_in.at[e, row],
                s_fold.at[e],
                r_fold.at[e],
            )
            odd_in[e, row] = back_out[j, 0, four(row)]

    for e in range(2):
        await_row(odd_in, r_fold, e)
    across(odd_in, even_out, ((1,), (1,)))
    for e in range(2):
        send_row(
            lambda to: even_out.at[e, to], fold_in.at[e, row], s_ret.at[e], r_ret.at[e]
        )
        fold_in[e, row] = even_out[e, row]
    for e in range(2):
        await_row(fold_in, r_ret, e)
        back_out[e, 0] = back_out[e, 0] + fold_in[e].reshape(COLS, 2, 8, 128)
        send_col(back_out, back_in, s_back, r_back, e, 0)

    @pl.loop(0, CHUNKS)
    def _(s):
        j = (s + 2) % CHUNKS
        await_col(back_in, r_back, j, 1)

        @pl.when(j < 2)
        def _():
            await_col(back_in, r_back, j, 0)

        data = jnp.concatenate(
            [
                jnp.stack([back_in[j, 0, :, q], back_in[j, 1, :, q]], 1).reshape(M, 128)
                for q in range(2)
            ],
            0,
        )
        back_y = product((full[0], full[1]), split(data), ((1,), (0,)))
        for q in range(2):
            for r in range(ROWS):
                last_out[j, r, q] = back_y[q * N + r * 32 : q * N + r * 32 + 32]
        send_row(lambda to: last_out.at[j, to], last_in.at[j, row], s_last.at[j], r_last.at[j])
        last_in[j, row] = last_out[j, row]

    out[...] = jnp.zeros_like(out)

    @pl.loop(0, CHUNKS)
    def _(s):
        j = (s + 2) % CHUNKS
        await_row(last_in, r_last, j)
        parts = []
        for q in range(2):
            pieces = swap_groups([last_in[j, r, q] for r in range(ROWS)], 1)
            parts.append(jnp.concatenate(pieces, 0))
        data = jnp.concatenate(parts, 1)
        out[...] += product(split(data), (ztab[0, j], ztab[1, j]), ((1,), (1,)))

    @pl.loop(0, CHUNKS)
    def _(j):
        await_row(row_out, s_row, j)
        await_row(last_out, s_last, j)
        await_col(col_out, s_col, j, 1)
        await_col(back_out, s_back, j, 1)

    @pl.loop(0, 2)
    def _(e):
        await_col(col_out, s_col, e, 0)
        await_col(back_out, s_back, e, 0)
        await_row(even_in, s_even, e)
        await_row(odd_out, s_odd, e)
        await_row(odd_in, s_fold, e)
        await_row(even_out, s_ret, e)


def on_device(charge, green_spectrum):
    z_table, wave, bridge = tables()
    any_space = pl.BlockSpec(memory_space=pl.ANY)
    row_buffer = pltpu.VMEM((CHUNKS, ROWS, 2, 32, 128), jnp.float32)
    col_buffer = pltpu.VMEM((CHUNKS, 2, COLS, 2, 8, 128), jnp.float32)
    side_buffer = pltpu.VMEM((2, ROWS, 4, 2, 8, 128), jnp.float32)
    field = pl.pallas_call(
        body,
        out_shape=jax.ShapeDtypeStruct((8 * 32, N), jnp.float32),
        in_specs=[any_space] * 5,
        out_specs=pl.BlockSpec(memory_space=pltpu.VMEM),
        scratch_shapes=[
            pltpu.VMEM((8, 32, N), jnp.float32),
            pltpu.VMEM((32, 2, 2, 8, M), jnp.float32),
            pltpu.VMEM(z_table.shape, jnp.bfloat16),
            pltpu.VMEM((2, 2 * N, 2 * M), jnp.bfloat16),
            pltpu.VMEM((2, 2 * N, 2 * N), jnp.bfloat16),
            row_buffer, row_buffer, col_buffer, col_buffer, col_buffer, col_buffer,
            row_buffer, row_buffer,
            side_buffer, side_buffer, side_buffer, side_buffer, side_buffer,
            pltpu.SemaphoreType.DMA((9,)),
            pltpu.SemaphoreType.DMA((CHUNKS,)),
            pltpu.SemaphoreType.DMA((CHUNKS,)),
        ]
        + [pltpu.SemaphoreType.DMA((2 * CHUNKS,))] * 4
        + [pltpu.SemaphoreType.DMA((CHUNKS,))] * 2
        + [pltpu.SemaphoreType.DMA((2,))] * 8,
        compiler_params=pltpu.CompilerParams(
            collective_id=0, has_side_effects=True, vmem_limit_bytes=56 * 2**20
        ),
        name="poisson",
    )(charge, green_spectrum.reshape(32, 2, 2, 8, M), z_table, wave, bridge)
    return (field * (1.0 / M**3)).reshape(8, 32, N)


def solution(mesh):
    in_specs = (P("col", "row", None), P("row", "col", None))
    out_specs = P("col", "row", None)
    return jax.shard_map(
        on_device, mesh=mesh, in_specs=in_specs, out_specs=out_specs, check_vma=False
    )
```

```python
import functools
import math

import jax
import jax.numpy as jnp
import numpy as np
from jax import lax
from jax.experimental import pallas as pl
from jax.experimental.pallas import tpu as pltpu
from jax.sharding import PartitionSpec as P

M = 512
N = 256
ROWS = 8
COLS = 32
CHUNKS = 4
CW = M // ROWS // CHUNKS
MESH = pl.DeviceIdType.MESH


def halves(table):
    high = table.astype(jnp.bfloat16)
    low = (table - high.astype(np.float32)).astype(jnp.bfloat16)
    return np.stack([high, low])


def tables():
    turns = np.arange(N)[:, None] * np.arange(M)[None, :] % M
    angles = turns * (2.0 * np.pi / M)
    cosine, sine = np.cos(angles), np.sin(angles)
    parts = np.stack([cosine, -sine], 1).reshape(N, 2, ROWS, 2, CW, 2)
    z_table = parts.transpose(5, 3, 0, 1, 4, 2).reshape(CHUNKS, N, 2 * CW * ROWS)
    order = np.arange(N).reshape(ROWS, 2, CW).transpose(1, 2, 0).reshape(N)
    gap = 2 * (order[None, :] - order[:, None]) + 1
    bridge = 2.0 / N / (1.0 - np.exp(-2j * np.pi * gap / M))
    return (
        halves(z_table.astype(np.float32)),
        halves(np.stack([cosine, sine]).astype(np.float32)),
        halves(np.stack([bridge.real, bridge.imag]).astype(np.float32)),
    )


def split(value):
    high = value.astype(jnp.bfloat16)
    low = (value - high.astype(jnp.float32)).astype(jnp.bfloat16)
    return high, low


def product(left, right, dims):
    def one(a, b):
        return lax.dot_general(a, b, (dims, ((), ())), preferred_element_type=jnp.float32)

    return one(left[0], right[0]) + (one(left[0], right[1]) + one(left[1], right[0]))


def swap_groups(parts, width):
    parts = list(parts)
    count = len(parts)
    lanes = parts[0].shape[-1]
    step = 1
    while step < count:
        shift = step * width
        lane = lax.broadcasted_iota(jnp.int32, parts[0].shape, len(parts[0].shape) - 1)
        upper = (lane // shift) % 2 == 1
        axis = len(parts[0].shape) - 1
        for i in range(count):
            if i & step:
                continue
            one, two = parts[i], parts[i | step]
            parts[i] = jnp.where(upper, pltpu.roll(two, shift, axis), one)
            parts[i | step] = jnp.where(upper, two, pltpu.roll(one, lanes - shift, axis))
        step *= 2
    return parts


def body(
    charge, green, ztab_h, wave_h, bridge_h, out, cells, gvm, ztab, full, bridge,
    row_out, row_in, col_out, col_in, back_out, back_in, last_out, last_in,
    even_in, odd_out, odd_in, even_out, fold_in, load,
    s_row, r_row, s_col, r_col, s_back, r_back, s_last, r_last,
    s_even, r_even, s_odd, r_odd, s_fold, r_fold, s_ret, r_ret,
):
    row, col = lax.axis_index("row"), lax.axis_index("col")
    barrier = pltpu.get_barrier_semaphore()
    low, high = pl.ds(0, N), pl.ds(N, N)
    left, right = pl.ds(0, M), pl.ds(M, M)
    pairs = [
        (charge, cells),
        (ztab_h, ztab),
        (wave_h.at[:, 0], full.at[:, low, left]),
        (wave_h.at[:, 0], full.at[:, high, right]),
        (wave_h.at[:, 1], full.at[:, high, left]),
        (bridge_h.at[:, 0], bridge.at[:, low, low]),
        (bridge_h.at[:, 0], bridge.at[:, high, high]),
        (bridge_h.at[:, 1], bridge.at[:, low, high]),
        (green, gvm),
    ]
    loads = [
        pltpu.make_async_copy(src, dst, load.at[k]) for k, (src, dst) in enumerate(pairs)
    ]

    def row_peer(k):
        return (row + k) % ROWS

    def col_peer(k):
        return (col + k) % COLS

    @pl.loop(1, COLS)
    def _(k):
        pl.semaphore_signal(barrier, inc=1, device_id={"col": col_peer(k)}, device_id_type=MESH)

    @pl.loop(1, ROWS)
    def _(k):
        pl.semaphore_signal(barrier, inc=1, device_id={"row": row_peer(k)}, device_id_type=MESH)

    for one in loads:
        one.start()

    def send_row(source, target, s_sem, r_sem):
        @pl.loop(1, ROWS)
        def _(k):
            to = row_peer(k)
            pltpu.make_async_remote_copy(
                src_ref=source(to),
                dst_ref=target,
                send_sem=s_sem,
                recv_sem=r_sem,
                device_id={"row": to},
                device_id_type=MESH,
            ).start()

    def send_col(source, target, s_sem, r_sem, j, half):
        target[j, half, col] = source[j, half, col]

        @pl.loop(1, COLS)
        def _(k):
            to = col_peer(k)
            pltpu.make_async_remote_copy(
                src_ref=source.at[j, half, to],
                dst_ref=target.at[j, half, col],
                send_sem=s_sem.at[2 * j + half],
                recv_sem=r_sem.at[2 * j + half],
                device_id={"col": to},
                device_id_type=MESH,
            ).start()

    def await_bytes(view, sem):
        pltpu.make_async_copy(view, view, sem).wait()

    def await_row(ref, sem, j):
        await_bytes(ref.at[j, pl.ds(0, ROWS - 1)], sem.at[j])

    def await_col(ref, sem, j, half):
        await_bytes(ref.at[j, half, pl.ds(0, COLS - 1)], sem.at[2 * j + half])

    loads[0].wait()
    loads[1].wait()
    cells_h, cells_l = split(cells[...].reshape(8 * 32, N))

    @pl.loop(0, CHUNKS)
    def _(j):
        along_z = product((cells_h, cells_l), (ztab[0, j], ztab[1, j]), ((1,), (0,)))
        for q in range(2):
            block = along_z[:, q * 128 : q * 128 + 128]
            pieces = swap_groups([block[x * 32 : x * 32 + 32] for x in range(8)], 1)
            for r in range(ROWS):
                row_out[j, r, q] = pieces[r]

    pl.semaphore_wait(barrier, ROWS - 1 + COLS - 1)

    @pl.loop(0, CHUNKS)
    def _(j):
        send_row(lambda to: row_out.at[j, to], row_in.at[j, row], s_row.at[j], r_row.at[j])
        row_in[j, row] = row_out[j, row]

    for one in loads[2:8]:
        one.wait()
    full[:, 0:N, M:] = -full[:, N:, 0:M]
    bridge[:, N:, 0:N] = -bridge[:, 0:N, N:]

    @pl.loop(0, CHUNKS)
    def _(j):
        await_row(row_in, r_row, j)
        data = jnp.concatenate([row_in[j, :, q].reshape(N, 128) for q in range(2)], 0)
        along_y = product(split(data.T), (full[0], full[1]), ((1,), (0,)))
        for v in range(8):
            q, top = v // 4, v % 4
            pieces = swap_groups(
                [along_y[i * 8 : i * 8 + 8, v * 128 : v * 128 + 128] for i in range(16)], 8
            )
            for g in range(16):
                col_out[j, g % 2, top * 8 + g // 2, q] = pieces[g]

        @pl.when(j < 2)
        def _():
            send_col(col_out, col_in, s_col, r_col, j, 0)

        @pl.when(j == 1)
        def _():
            send_col(col_out, col_in, s_col, r_col, 0, 1)

        @pl.when(j >= 1)
        def _():
            send_col(col_out, col_in, s_col, r_col, j, 1)

    loads[8].wait()
    for e in range(2):
        back_in[2 + e, 0] = jnp.zeros_like(back_in[2 + e, 0])

    def four(index):
        return pl.ds(index * 4, 4)

    def across(source, target, dims):
        parts = []
        for q in range(2):
            for e in range(2):
                pieces = [source[e, r, :, q].reshape(32, 128) for r in range(ROWS)]
                parts.append(jnp.concatenate(swap_groups(pieces, 1), 0))
        data = jnp.concatenate(parts, 1)
        moved = product(split(data), (bridge[0], bridge[1]), dims)
        for v in range(4):
            q, e = v // 2, v % 2
            block = moved[:, v * 128 : v * 128 + 128]
            pieces = swap_groups([block[k * 32 : k * 32 + 32] for k in range(8)], 1)
            for r in range(ROWS):
                target[e, r, :, q] = pieces[r].reshape(4, 8, 128)

    @pl.loop(0, 2 * CHUNKS)
    def _(s):
        j = s // 4 * 2 + s % 2
        half = s % 4 // 2
        e = s % 2

        @pl.when(s == 2)
        def _():
            for k in range(2):
                await_row(even_in, r_even, k)
            across(even_in, odd_out, ((1,), (0,)))
            for k in range(2):
                send_row(
                    lambda to: odd_out.at[k, to],
                    col_in.at[2 + k, 0, four(row)],
                    s_odd.at[k],
                    r_odd.at[k],
                )
                col_in[2 + k, 0, four(row)] = odd_out[k, row]

        @pl.when((j < 2) | (half == 1))
        def _():
            await_col(col_in, r_col, j, half)

        @pl.when((j >= 2) & (half == 0))
        def _():
            await_row(odd_in, r_odd, e)

        @pl.when(s < 2)
        def _():
            send_row(
                lambda to: col_in.at[e, 0, four(to)],
                even_in.at[e, row],
                s_even.at[e],
                r_even.at[e],
            )
            even_in[e, row] = col_in[e, 0, four(row)]

        data = jnp.concatenate([col_in[j, half, :, q].reshape(N, 128) for q in range(2)], 0)
        spectrum = product(split(data.T), (full[0], full[1]), ((1,), (0,)))
        weight = gvm[pl.ds(e * CW, CW), j // 2, half].reshape(128, M)
        scaled = spectrum * jnp.concatenate([weight, weight], 1)
        along_x = product(split(scaled), (full[0], full[1]), ((1,), (1,)))
        for v in range(4):
            q, top = v // 2, v % 2
            pieces = swap_groups(
                [along_x[i * 8 : i * 8 + 8, v * 128 : v * 128 + 128] for i in range(16)], 8
            )
            for g in range(16):
                back_out[j, half, top * 16 + g, q] = pieces[g]

        @pl.when(half == 1)
        def _():
            send_col(back_out, back_in, s_back, r_back, j, half)

        @pl.when((j >= 2) & (half == 0))
        def _():
            send_row(
                lambda to: back_out.at[j, 0, four(to)],
                odd_in.at[e, row],
                s_fold.at[e],
                r_fold.at[e],
            )
            odd_in[e, row] = back_out[j, 0, four(row)]

    for e in range(2):
        await_row(odd_in, r_fold, e)
    across(odd_in, even_out, ((1,), (1,)))
    for e in range(2):
        send_row(
            lambda to: even_out.at[e, to], fold_in.at[e, row], s_ret.at[e], r_ret.at[e]
        )
        fold_in[e, row] = even_out[e, row]
    for e in range(2):
        await_row(fold_in, r_ret, e)
        back_out[e, 0] = back_out[e, 0] + fold_in[e].reshape(COLS, 2, 8, 128)
        send_col(back_out, back_in, s_back, r_back, e, 0)

    @pl.loop(0, CHUNKS)
    def _(s):
        j = (s + 2) % CHUNKS
        await_col(back_in, r_back, j, 1)

        @pl.when(j < 2)
        def _():
            await_col(back_in, r_back, j, 0)

        data = jnp.concatenate(
            [
                jnp.stack([back_in[j, 0, :, q], back_in[j, 1, :, q]], 1).reshape(M, 128)
                for q in range(2)
            ],
            0,
        )
        back_y = product((full[0], full[1]), split(data), ((1,), (0,)))
        for q in range(2):
            for r in range(ROWS):
                last_out[j, r, q] = back_y[q * N + r * 32 : q * N + r * 32 + 32]
        send_row(lambda to: last_out.at[j, to], last_in.at[j, row], s_last.at[j], r_last.at[j])
        last_in[j, row] = last_out[j, row]

    out[...] = jnp.zeros_like(out)

    @pl.loop(0, CHUNKS)
    def _(s):
        j = (s + 2) % CHUNKS
        await_row(last_in, r_last, j)
        parts = []
        for q in range(2):
            pieces = swap_groups([last_in[j, r, q] for r in range(ROWS)], 1)
            parts.append(jnp.concatenate(pieces, 0))
        data = jnp.concatenate(parts, 1)
        out[...] += product(split(data), (ztab[0, j], ztab[1, j]), ((1,), (1,)))

    @pl.loop(0, CHUNKS)
    def _(j):
        await_row(row_out, s_row, j)
        await_row(last_out, s_last, j)
        await_col(col_out, s_col, j, 1)
        await_col(back_out, s_back, j, 1)

    @pl.loop(0, 2)
    def _(e):
        await_col(col_out, s_col, e, 0)
        await_col(back_out, s_back, e, 0)
        await_row(even_in, s_even, e)
        await_row(odd_out, s_odd, e)
        await_row(odd_in, s_fold, e)
        await_row(even_out, s_ret, e)


def on_device(charge, green_spectrum):
    z_table, wave, bridge = tables()
    any_space = pl.BlockSpec(memory_space=pl.ANY)
    row_buffer = pltpu.VMEM((CHUNKS, ROWS, 2, 32, 128), jnp.float32)
    col_buffer = pltpu.VMEM((CHUNKS, 2, COLS, 2, 8, 128), jnp.float32)
    side_buffer = pltpu.VMEM((2, ROWS, 4, 2, 8, 128), jnp.float32)
    field = pl.pallas_call(
        body,
        out_shape=jax.ShapeDtypeStruct((8 * 32, N), jnp.float32),
        in_specs=[any_space] * 5,
        out_specs=pl.BlockSpec(memory_space=pltpu.VMEM),
        scratch_shapes=[
            pltpu.VMEM((8, 32, N), jnp.float32),
            pltpu.VMEM((32, 2, 2, 8, M), jnp.float32),
            pltpu.VMEM(z_table.shape, jnp.bfloat16),
            pltpu.VMEM((2, 2 * N, 2 * M), jnp.bfloat16),
            pltpu.VMEM((2, 2 * N, 2 * N), jnp.bfloat16),
            row_buffer, row_buffer, col_buffer, col_buffer, col_buffer, col_buffer,
            row_buffer, row_buffer,
            side_buffer, side_buffer, side_buffer, side_buffer, side_buffer,
            pltpu.SemaphoreType.DMA((9,)),
            pltpu.SemaphoreType.DMA((CHUNKS,)),
            pltpu.SemaphoreType.DMA((CHUNKS,)),
        ]
        + [pltpu.SemaphoreType.DMA((2 * CHUNKS,))] * 4
        + [pltpu.SemaphoreType.DMA((CHUNKS,))] * 2
        + [pltpu.SemaphoreType.DMA((2,))] * 8,
        compiler_params=pltpu.CompilerParams(
            collective_id=0, has_side_effects=True, vmem_limit_bytes=54800 * 2**10
        ),
        name="poisson",
    )(charge, green_spectrum.reshape(32, 2, 2, 8, M), z_table, wave, bridge)
    return (field * (1.0 / M**3)).reshape(8, 32, N)


def solution(mesh):
    in_specs = (P("col", "row", None), P("row", "col", None))
    out_specs = P("col", "row", None)
    return jax.shard_map(
        on_device, mesh=mesh, in_specs=in_specs, out_specs=out_specs, check_vma=False
    )
```

```python
import functools
import math

import jax
import jax.numpy as jnp
import numpy as np
from jax import lax
from jax.experimental import pallas as pl
from jax.experimental.pallas import tpu as pltpu
from jax.sharding import PartitionSpec as P

M = 512
N = 256
ROWS = 8
COLS = 32
CHUNKS = 4
CW = M // ROWS // CHUNKS
MESH = pl.DeviceIdType.MESH


def halves(table):
    high = table.astype(jnp.bfloat16)
    low = (table - high.astype(np.float32)).astype(jnp.bfloat16)
    return np.stack([high, low])


def tables():
    turns = np.arange(N)[:, None] * np.arange(M)[None, :] % M
    angles = turns * (2.0 * np.pi / M)
    cosine, sine = np.cos(angles), np.sin(angles)
    parts = np.stack([cosine, -sine], 1).reshape(N, 2, ROWS, 2, CW, 2)
    z_table = parts.transpose(5, 3, 0, 1, 4, 2).reshape(CHUNKS, N, 2 * CW * ROWS)
    order = np.arange(N).reshape(ROWS, 2, CW).transpose(1, 2, 0).reshape(N)
    gap = 2 * (order[None, :] - order[:, None]) + 1
    bridge = 2.0 / N / (1.0 - np.exp(-2j * np.pi * gap / M))
    return (
        halves(z_table.astype(np.float32)),
        halves(np.stack([cosine, sine]).astype(np.float32)),
        halves(np.stack([bridge.real, bridge.imag]).astype(np.float32)),
    )


def split(value):
    high = value.astype(jnp.bfloat16)
    low = (value - high.astype(jnp.float32)).astype(jnp.bfloat16)
    return high, low


def product(left, right, dims):
    def one(a, b):
        return lax.dot_general(a, b, (dims, ((), ())), preferred_element_type=jnp.float32)

    return one(left[0], right[0]) + (one(left[0], right[1]) + one(left[1], right[0]))


def swap_groups(parts, width):
    parts = list(parts)
    count = len(parts)
    lanes = parts[0].shape[-1]
    step = 1
    while step < count:
        shift = step * width
        lane = lax.broadcasted_iota(jnp.int32, parts[0].shape, len(parts[0].shape) - 1)
        upper = (lane // shift) % 2 == 1
        axis = len(parts[0].shape) - 1
        for i in range(count):
            if i & step:
                continue
            one, two = parts[i], parts[i | step]
            parts[i] = jnp.where(upper, pltpu.roll(two, shift, axis), one)
            parts[i | step] = jnp.where(upper, two, pltpu.roll(one, lanes - shift, axis))
        step *= 2
    return parts


def body(
    charge, green, ztab_h, wave_h, bridge_h, out, cells, gvm, ztab, full, bridge,
    row_out, row_in, col_out, col_in, back_out, back_in, last_out, last_in,
    even_in, odd_out, odd_in, even_out, fold_in, load,
    s_row, r_row, s_col, r_col, s_back, r_back, s_last, r_last,
    s_even, r_even, s_odd, r_odd, s_fold, r_fold, s_ret, r_ret,
):
    row, col = lax.axis_index("row"), lax.axis_index("col")
    barrier = pltpu.get_barrier_semaphore()
    low, high = pl.ds(0, N), pl.ds(N, N)
    left, right = pl.ds(0, M), pl.ds(M, M)
    pairs = [
        (charge, cells),
        (ztab_h, ztab),
        (wave_h.at[:, 0], full.at[:, low, left]),
        (wave_h.at[:, 0], full.at[:, high, right]),
        (wave_h.at[:, 1], full.at[:, high, left]),
        (bridge_h.at[:, 0], bridge.at[:, low, low]),
        (bridge_h.at[:, 0], bridge.at[:, high, high]),
        (bridge_h.at[:, 1], bridge.at[:, low, high]),
        (green, gvm),
    ]
    loads = [
        pltpu.make_async_copy(src, dst, load.at[k]) for k, (src, dst) in enumerate(pairs)
    ]

    def row_peer(k):
        return (row + k) % ROWS

    def col_peer(k):
        ahead, behind = (k + 1) // 2, COLS - k // 2
        return (col + k % 2 * ahead + (1 - k % 2) * behind) % COLS

    @pl.loop(1, COLS)
    def _(k):
        pl.semaphore_signal(barrier, inc=1, device_id={"col": col_peer(k)}, device_id_type=MESH)

    @pl.loop(1, ROWS)
    def _(k):
        pl.semaphore_signal(barrier, inc=1, device_id={"row": row_peer(k)}, device_id_type=MESH)

    for one in loads:
        one.start()

    def send_row(source, target, s_sem, r_sem):
        @pl.loop(1, ROWS)
        def _(k):
            to = row_peer(k)
            pltpu.make_async_remote_copy(
                src_ref=source(to),
                dst_ref=target,
                send_sem=s_sem,
                recv_sem=r_sem,
                device_id={"row": to},
                device_id_type=MESH,
            ).start()

    def send_col(source, target, s_sem, r_sem, j, half):
        target[j, half, col] = source[j, half, col]

        @pl.loop(1, COLS)
        def _(k):
            to = col_peer(k)
            pltpu.make_async_remote_copy(
                src_ref=source.at[j, half, to],
                dst_ref=target.at[j, half, col],
                send_sem=s_sem.at[2 * j + half],
                recv_sem=r_sem.at[2 * j + half],
                device_id={"col": to},
                device_id_type=MESH,
            ).start()

    def await_bytes(view, sem):
        pltpu.make_async_copy(view, view, sem).wait()

    def await_row(ref, sem, j):
        await_bytes(ref.at[j, pl.ds(0, ROWS - 1)], sem.at[j])

    def await_col(ref, sem, j, half):
        await_bytes(ref.at[j, half, pl.ds(0, COLS - 1)], sem.at[2 * j + half])

    loads[0].wait()
    loads[1].wait()
    cells_h, cells_l = split(cells[...].reshape(8 * 32, N))

    @pl.loop(0, CHUNKS)
    def _(j):
        along_z = product((cells_h, cells_l), (ztab[0, j], ztab[1, j]), ((1,), (0,)))
        for q in range(2):
            block = along_z[:, q * 128 : q * 128 + 128]
            pieces = swap_groups([block[x * 32 : x * 32 + 32] for x in range(8)], 1)
            for r in range(ROWS):
                row_out[j, r, q] = pieces[r]

    pl.semaphore_wait(barrier, ROWS - 1 + COLS - 1)

    @pl.loop(0, CHUNKS)
    def _(j):
        send_row(lambda to: row_out.at[j, to], row_in.at[j, row], s_row.at[j], r_row.at[j])
        row_in[j, row] = row_out[j, row]

    for one in loads[2:8]:
        one.wait()
    full[:, 0:N, M:] = -full[:, N:, 0:M]
    bridge[:, N:, 0:N] = -bridge[:, 0:N, N:]

    @pl.loop(0, CHUNKS)
    def _(j):
        await_row(row_in, r_row, j)
        data = jnp.concatenate([row_in[j, :, q].reshape(N, 128) for q in range(2)], 0)
        along_y = product(split(data.T), (full[0], full[1]), ((1,), (0,)))
        for v in range(8):
            q, top = v // 4, v % 4
            pieces = swap_groups(
                [along_y[i * 8 : i * 8 + 8, v * 128 : v * 128 + 128] for i in range(16)], 8
            )
            for g in range(16):
                col_out[j, g % 2, top * 8 + g // 2, q] = pieces[g]

        @pl.when(j < 2)
        def _():
            send_col(col_out, col_in, s_col, r_col, j, 0)

        @pl.when(j == 1)
        def _():
            send_col(col_out, col_in, s_col, r_col, 0, 1)

        @pl.when(j >= 1)
        def _():
            send_col(col_out, col_in, s_col, r_col, j, 1)

    loads[8].wait()
    for e in range(2):
        back_in[2 + e, 0] = jnp.zeros_like(back_in[2 + e, 0])

    def four(index):
        return pl.ds(index * 4, 4)

    def across(source, target, dims):
        parts = []
        for q in range(2):
            for e in range(2):
                pieces = [source[e, r, :, q].reshape(32, 128) for r in range(ROWS)]
                parts.append(jnp.concatenate(swap_groups(pieces, 1), 0))
        data = jnp.concatenate(parts, 1)
        moved = product(split(data), (bridge[0], bridge[1]), dims)
        for v in range(4):
            q, e = v // 2, v % 2
            block = moved[:, v * 128 : v * 128 + 128]
            pieces = swap_groups([block[k * 32 : k * 32 + 32] for k in range(8)], 1)
            for r in range(ROWS):
                target[e, r, :, q] = pieces[r].reshape(4, 8, 128)

    @pl.loop(0, 2 * CHUNKS)
    def _(s):
        j = s // 4 * 2 + s % 2
        half = s % 4 // 2
        e = s % 2

        @pl.when(s == 2)
        def _():
            for k in range(2):
                await_row(even_in, r_even, k)
            across(even_in, odd_out, ((1,), (0,)))
            for k in range(2):
                send_row(
                    lambda to: odd_out.at[k, to],
                    col_in.at[2 + k, 0, four(row)],
                    s_odd.at[k],
                    r_odd.at[k],
                )
                col_in[2 + k, 0, four(row)] = odd_out[k, row]

        @pl.when((j < 2) | (half == 1))
        def _():
            await_col(col_in, r_col, j, half)

        @pl.when((j >= 2) & (half == 0))
        def _():
            await_row(odd_in, r_odd, e)

        @pl.when(s < 2)
        def _():
            send_row(
                lambda to: col_in.at[e, 0, four(to)],
                even_in.at[e, row],
                s_even.at[e],
                r_even.at[e],
            )
            even_in[e, row] = col_in[e, 0, four(row)]

        data = jnp.concatenate([col_in[j, half, :, q].reshape(N, 128) for q in range(2)], 0)
        spectrum = product(split(data.T), (full[0], full[1]), ((1,), (0,)))
        weight = gvm[pl.ds(e * CW, CW), j // 2, half].reshape(128, M)
        scaled = spectrum * jnp.concatenate([weight, weight], 1)
        along_x = product(split(scaled), (full[0], full[1]), ((1,), (1,)))
        for v in range(4):
            q, top = v // 2, v % 2
            pieces = swap_groups(
                [along_x[i * 8 : i * 8 + 8, v * 128 : v * 128 + 128] for i in range(16)], 8
            )
            for g in range(16):
                back_out[j, half, top * 16 + g, q] = pieces[g]

        @pl.when(half == 1)
        def _():
            send_col(back_out, back_in, s_back, r_back, j, half)

        @pl.when((j >= 2) & (half == 0))
        def _():
            send_row(
                lambda to: back_out.at[j, 0, four(to)],
                odd_in.at[e, row],
                s_fold.at[e],
                r_fold.at[e],
            )
            odd_in[e, row] = back_out[j, 0, four(row)]

    for e in range(2):
        await_row(odd_in, r_fold, e)
    across(odd_in, even_out, ((1,), (1,)))
    for e in range(2):
        send_row(
            lambda to: even_out.at[e, to], fold_in.at[e, row], s_ret.at[e], r_ret.at[e]
        )
        fold_in[e, row] = even_out[e, row]
    for e in range(2):
        await_row(fold_in, r_ret, e)
        back_out[e, 0] = back_out[e, 0] + fold_in[e].reshape(COLS, 2, 8, 128)
        send_col(back_out, back_in, s_back, r_back, e, 0)

    @pl.loop(0, CHUNKS)
    def _(s):
        j = (s + 2) % CHUNKS
        await_col(back_in, r_back, j, 1)

        @pl.when(j < 2)
        def _():
            await_col(back_in, r_back, j, 0)

        data = jnp.concatenate(
            [
                jnp.stack([back_in[j, 0, :, q], back_in[j, 1, :, q]], 1).reshape(M, 128)
                for q in range(2)
            ],
            0,
        )
        back_y = product((full[0], full[1]), split(data), ((1,), (0,)))
        for q in range(2):
            for r in range(ROWS):
                last_out[j, r, q] = back_y[q * N + r * 32 : q * N + r * 32 + 32]
        send_row(lambda to: last_out.at[j, to], last_in.at[j, row], s_last.at[j], r_last.at[j])
        last_in[j, row] = last_out[j, row]

    out[...] = jnp.zeros_like(out)

    @pl.loop(0, CHUNKS)
    def _(s):
        j = (s + 2) % CHUNKS
        await_row(last_in, r_last, j)
        parts = []
        for q in range(2):
            pieces = swap_groups([last_in[j, r, q] for r in range(ROWS)], 1)
            parts.append(jnp.concatenate(pieces, 0))
        data = jnp.concatenate(parts, 1)
        out[...] += product(split(data), (ztab[0, j], ztab[1, j]), ((1,), (1,)))

    @pl.loop(0, CHUNKS)
    def _(j):
        await_row(row_out, s_row, j)
        await_row(last_out, s_last, j)
        await_col(col_out, s_col, j, 1)
        await_col(back_out, s_back, j, 1)

    @pl.loop(0, 2)
    def _(e):
        await_col(col_out, s_col, e, 0)
        await_col(back_out, s_back, e, 0)
        await_row(even_in, s_even, e)
        await_row(odd_out, s_odd, e)
        await_row(odd_in, s_fold, e)
        await_row(even_out, s_ret, e)


def on_device(charge, green_spectrum):
    z_table, wave, bridge = tables()
    any_space = pl.BlockSpec(memory_space=pl.ANY)
    row_buffer = pltpu.VMEM((CHUNKS, ROWS, 2, 32, 128), jnp.float32)
    col_buffer = pltpu.VMEM((CHUNKS, 2, COLS, 2, 8, 128), jnp.float32)
    side_buffer = pltpu.VMEM((2, ROWS, 4, 2, 8, 128), jnp.float32)
    field = pl.pallas_call(
        body,
        out_shape=jax.ShapeDtypeStruct((8 * 32, N), jnp.float32),
        in_specs=[any_space] * 5,
        out_specs=pl.BlockSpec(memory_space=pltpu.VMEM),
        scratch_shapes=[
            pltpu.VMEM((8, 32, N), jnp.float32),
            pltpu.VMEM((32, 2, 2, 8, M), jnp.float32),
            pltpu.VMEM(z_table.shape, jnp.bfloat16),
            pltpu.VMEM((2, 2 * N, 2 * M), jnp.bfloat16),
            pltpu.VMEM((2, 2 * N, 2 * N), jnp.bfloat16),
            row_buffer, row_buffer, col_buffer, col_buffer, col_buffer, col_buffer,
            row_buffer, row_buffer,
            side_buffer, side_buffer, side_buffer, side_buffer, side_buffer,
            pltpu.SemaphoreType.DMA((9,)),
            pltpu.SemaphoreType.DMA((CHUNKS,)),
            pltpu.SemaphoreType.DMA((CHUNKS,)),
        ]
        + [pltpu.SemaphoreType.DMA((2 * CHUNKS,))] * 4
        + [pltpu.SemaphoreType.DMA((CHUNKS,))] * 2
        + [pltpu.SemaphoreType.DMA((2,))] * 8,
        compiler_params=pltpu.CompilerParams(
            collective_id=0, has_side_effects=True, vmem_limit_bytes=54800 * 2**10
        ),
        name="poisson",
    )(charge, green_spectrum.reshape(32, 2, 2, 8, M), z_table, wave, bridge)
    return (field * (1.0 / M**3)).reshape(8, 32, N)


def solution(mesh):
    in_specs = (P("col", "row", None), P("row", "col", None))
    out_specs = P("col", "row", None)
    return jax.shard_map(
        on_device, mesh=mesh, in_specs=in_specs, out_specs=out_specs, check_vma=False
    )
```
